32 devices in a mesh: mb: 4 (over z), tp: 2 (over y), dp: 4 (over x, core).
Axes of the slice: x: 2, y: 2, z: 4, core: 2. Of those that a mesh axis runs over, the one named last changes fastest.
Arguments:
- hidden: bfloat16 [4, 8, 512, 7168], P('dp', 'mb', None, 'tp'), may hold values from -6 to 6
- latent: bfloat16 [4, 8, 512, 512], P('dp', 'mb', None, 'tp'), may hold values from -6 to 6
- out_grad: bfloat16 [4, 8, 512, 16384], P('dp', 'mb', None, 'tp'), may hold values from -0.059814453 to 0.059814453
- up_weight: bfloat16 [512, 16384], P(None, 'tp'), may hold values from -0.046875 to 0.046875
- mb_tokens: int32 [4, 8], P('dp'), may hold values from 128 to 512, as said below
- slot_mb: int32 [4, 8], P('dp', 'mb'), may hold values from 0 to 7, each once within a row
Outputs:
- up_grad: float32 [512, 16384], P(('mb', 'dp'), 'tp')
- running_down: float32 [4, 7168, 512], P('mb', 'tp', 'dp')
The draws below stay inside these ranges and needn't reach their ends.
Inputs may be any that keep to these rules, and one draw needn't show every extreme that they name: `mb_tokens`: each count is a multiple of 128; in every group some microbatch has exactly 512 tokens. `slot_mb`: each row is a permutation of the microbatch numbers.
All inputs are finite; a program needn't handle non-finite values.
Results may differ from the reference program's by a relative error of at most 0.005.
Values may be sent and summed in bfloat16 or wider, within the bound.
A program may use at most 128 MiB of HBM per device.

```python
import jax
import jax.numpy as jnp
from jax import lax

D = 7168
R = 512
COLS = 16384
TOKBLOCK = 128
CAP = 512
SLOTS = 2
MICRO = 8
GROUPS = 4
N_MB = 4


def draw_mb_tokens(key, part):
    first_key, second_key = jax.random.split(jax.random.fold_in(key, 11))
    blocks = jax.random.randint(first_key, (GROUPS, MICRO), 1, CAP // TOKBLOCK + 1)
    chosen = jax.random.randint(second_key, (GROUPS, 1), 0, MICRO)
    blocks = jnp.where(jnp.arange(MICRO)[None, :] == chosen, CAP // TOKBLOCK, blocks)
    return (blocks * TOKBLOCK).astype(jnp.int32)


def block_scale(own_key, dims, cuts, smallest, top_value):
    level, own = 1.0, jax.random.fold_in(own_key, 6)
    for axis_at, shards_of in cuts:
        steps = jnp.exp(jax.random.uniform(jax.random.fold_in(own, axis_at), (shards_of,), jnp.float32, smallest / len(cuts), top_value / len(cuts)))
        level = level * jnp.repeat(steps, dims[axis_at] // shards_of).reshape([-1 if axis == axis_at else 1 for axis in range(len(dims))])
    return level


def noise(rng, shape, scale, limit, cuts=(), kind=jnp.bfloat16):
    values = jax.random.normal(rng, shape, jnp.float32) * scale
    if len(cuts) > 0:
        values = block_scale(rng, shape, cuts, -0.22, 0.18) * values
    return jnp.clip(values, min=-limit, max=limit).astype(kind)


def setup_inputs(seed: int = 0) -> dict:
    key_of = jax.random.split(jax.random.key(seed), 7)
    return {
        "hidden": noise(key_of[0], (GROUPS, MICRO, CAP, D), 1.0, 6.0, ((0, 4), (1, 4), (3, 2))),
        "latent": noise(key_of[1], (GROUPS, MICRO, CAP, R), 1.0, 6.0, ((0, 4), (1, 4), (3, 2))),
        "out_grad": noise(key_of[2], (GROUPS, MICRO, CAP, COLS), 0.01, 0.059814453, ((0, 4), (1, 4), (3, 2))),
        "up_weight": noise(key_of[3], (R, COLS), COLS ** -0.5, 0.046875, ((1, 2),)),
        "mb_tokens": draw_mb_tokens(jax.random.fold_in(key_of[6], 71), 0),
        "slot_mb": jax.vmap(lambda own: jax.random.permutation(own, MICRO))(jax.random.split(key_of[5], GROUPS)).reshape((GROUPS, MICRO)).astype(jnp.int32),
    }


def reference(hidden, latent, out_grad, up_weight, mb_tokens, slot_mb):
    counts = jnp.take_along_axis(mb_tokens, slot_mb, axis=1).reshape(-1)
    owners = jnp.tile(jnp.arange(MICRO, dtype=jnp.int32) // SLOTS, GROUPS)
    positions = jnp.arange(CAP, dtype=jnp.int32)

    def accumulate(carry, inputs_now):
        up_total, down_owner = carry
        hidden_rows, latent_rows, grad_rows, length, owner_id = inputs_now
        masked = jnp.where((positions < length)[:, None], grad_rows, jnp.zeros((), grad_rows.dtype))
        latent_grad = jnp.dot(masked, up_weight.T, preferred_element_type=jnp.float32).astype(jnp.bfloat16)
        up_total = up_total + jnp.dot(latent_rows.T, masked, preferred_element_type=jnp.float32)
        down_term = jnp.dot(hidden_rows.T, latent_grad, preferred_element_type=jnp.float32)
        down_owner = down_owner.at[owner_id].add(down_term)
        return (up_total, down_owner), None

    start_state = (jnp.zeros((R, COLS), jnp.float32), jnp.zeros((N_MB, D, R), jnp.float32))
    sequence = (hidden.reshape(-1, CAP, D), latent.reshape(-1, CAP, R), out_grad.reshape(-1, CAP, COLS), counts, owners)
    (up_total, down_owner), unused = lax.scan(accumulate, start_state, sequence)
    return up_total, jnp.cumsum(down_owner, axis=0)
```

```python
import functools

import jax
import jax.numpy as jnp
from jax import lax
from jax.experimental import pallas as pl
from jax.experimental.pallas import tpu as pltpu
from jax.sharding import PartitionSpec as P

F32 = jnp.float32
BF16 = jnp.bfloat16
UP_CHUNKS = 8
DOWN_CHUNKS = 7


def bits_of(size):
    count = size.bit_length() - 1
    assert size == 1 << count, "axis size"
    return count


def kernel(sizes, hidden, latent, grad, weight, tokens, slots, up_out, run_out,
           grad_v, weight_v, hidden_v, lat_v, lat_t, lg_acc, lg_send, lg_recv, lg_t,
           up, up_r, dn, dn_r, pre_r, pre_s,
           grad_sem, weight_sem, hidden_sem, lat_sem, lat_ss, lat_rs, lg_ss, lg_rs,
           up_ss, up_rs, dn_ss, dn_rs, pre_ss, pre_rs):
    n_mb, n_tp, n_dp = sizes
    mb, tp, dp = (lax.axis_index(a) for a in ("mb", "tp", "dp"))
    up_chunks, slot_count, cap, width = grad_v.shape
    rows = slot_count * cap
    rank_part = lat_v.shape[-1]
    down_chunks, down_width = dn.shape[0], dn.shape[-1]

    steps = []
    for axis, index, size in (("dp", dp, n_dp), ("mb", mb, n_mb)):
        for k in range(bits_of(size)):
            bit = (index // (1 << k)) % 2
            steps.append((bit, {axis: index + (1 - 2 * bit) * (1 << k)}))
    n_dp_steps = bits_of(n_dp)
    tp_peers = [{"tp": (tp + s) % n_tp} for s in range(1, n_tp)]
    following, preceding = {"mb": (mb + 1) % n_mb}, {"mb": (mb + n_mb - 1) % n_mb}

    def grad_copy(c):
        return pltpu.make_async_copy(
            grad.at[0, :, :, pl.ds(pl.multiple_of(c * width, width), width)], grad_v.at[c], grad_sem.at[c])

    def weight_copy(c):
        return pltpu.make_async_copy(
            weight.at[:, pl.ds(pl.multiple_of(c * width, width), width)], weight_v.at[c % 2], weight_sem.at[c % 2])

    def hidden_copy(c):
        return pltpu.make_async_copy(
            hidden.at[0, :, :, pl.ds(pl.multiple_of(c * down_width, down_width), down_width)],
            hidden_v.at[c % 2], hidden_sem.at[c % 2])

    def remote(src, dst, ss, rs, to):
        return pltpu.make_async_remote_copy(
            src_ref=src, dst_ref=dst, send_sem=ss, recv_sem=rs,
            device_id=to, device_id_type=pl.DeviceIdType.MESH)

    own_latent = pltpu.make_async_copy(latent.at[0], lat_v.at[0], lat_sem)
    own_latent.start()
    for c in range(2):
        weight_copy(c).start()
        hidden_copy(c).start()

    @pl.loop(0, up_chunks)
    def _(c):
        grad_copy(c).start()

    barrier = pltpu.get_barrier_semaphore()
    greeted = [to for _, to in steps] + tp_peers + [following, preceding]
    for to in greeted:
        pl.semaphore_signal(barrier, inc=1, device_id=to, device_id_type=pl.DeviceIdType.MESH)
    pl.semaphore_wait(barrier, len(greeted))

    def lat_copy(s):
        return remote(latent.at[0], lat_v.at[s], lat_ss.at[s - 1], lat_rs.at[s - 1], tp_peers[s - 1])

    def lg_copy(s):
        return remote(lg_send, lg_recv.at[s - 1], lg_ss.at[s - 1], lg_rs.at[s - 1], tp_peers[s - 1])

    for s in range(1, n_tp):
        lat_copy(s).start()

    def up_copy(k, c):
        bit, to = steps[k]
        src = (up if k == 0 else up_r[k - 1]).at[c]
        index = (slice(None),) * (len(steps) - 1 - k) + (1 - bit,)
        return remote(src.at[index], up_r[k].at[c], up_ss.at[k, c], up_rs.at[k, c], to)

    def up_kept(k, c):
        bit, _ = steps[k]
        src = up if k == 0 else up_r[k - 1]
        return src[(c,) + (slice(None),) * (len(steps) - 1 - k) + (bit,)].astype(F32)

    def up_add(k, c):
        up_copy(k, c).wait_recv()
        return up_kept(k, c) + up_r[k][c].astype(F32)

    def up_pass(k, c):
        up_r[k][c] = up_add(k, c).astype(BF16)
        up_copy(k + 1, c).start()

    def dn_copy(k, c):
        bit, to = steps[k]
        src = (dn if k == 0 else dn_r[k - 1]).at[c]
        index = (slice(None),) * (n_dp_steps - 1 - k) + (1 - bit,)
        return remote(src.at[index], dn_r[k].at[c], dn_ss.at[k, c], dn_rs.at[k, c], to)

    def dn_add(k, c):
        bit, _ = steps[k]
        dn_copy(k, c).wait_recv()
        src = dn if k == 0 else dn_r[k - 1]
        kept = src[(c,) + (slice(None),) * (n_dp_steps - 1 - k) + (bit,)]
        return kept.astype(F32) + dn_r[k][c].astype(F32)

    def dn_pass(k, c):
        dn_r[k][c] = dn_add(k, c).astype(BF16)
        dn_copy(k + 1, c).start()

    def pre_copy(c):
        return remote(pre_s.at[c], pre_r.at[c], pre_ss.at[c], pre_rs.at[c], following)

    counts = [tokens[0, slots[0, s]] for s in range(slot_count)]

    def live(shape):
        row = lax.broadcasted_iota(jnp.int32, shape, 0)
        valid = row < counts[0]
        for s in range(1, slot_count):
            valid = valid | ((row >= s * cap) & (row < s * cap + counts[s]))
        return valid

    lg_acc[...] = jnp.zeros_like(lg_acc)

    @pl.loop(0, up_chunks)
    def _(c):
        grad_copy(c).wait()
        weight_copy(c).wait()
        lg_acc[...] += lax.dot_general(
            grad_v[c].reshape(rows, width), weight_v[c % 2], (((1,), (1,)), ((), ())),
            preferred_element_type=F32)

        @pl.when(c + 2 < up_chunks)
        def _():
            weight_copy(c + 2).start()

    lg_send[...] = lg_acc[...].astype(BF16)
    for s in range(1, n_tp):
        lg_copy(s).start()

    own_latent.wait()
    for s in range(1, n_tp):
        lat_copy(s).wait_recv()
    for s in range(n_tp):
        part = lat_v[s].reshape(rows, rank_part).astype(F32)
        part = jnp.where(live(part.shape), part, 0.0)
        home = (tp + n_tp - s) % n_tp
        lat_t[home] = part.T.astype(BF16)

    def up_first(c):
        up_pass(0, c)

    @pl.loop(0, up_chunks)
    def _(c):
        block = lax.dot_general(
            lat_t[...].reshape(n_tp * rank_part, rows), grad_v[c].reshape(rows, width),
            (((1,), (0,)), ((), ())), preferred_element_type=F32)
        up[c] = block.astype(BF16).reshape(up.shape[1:])
        up_copy(0, c).start()

        @pl.when(c > 0)
        def _():
            up_first(c - 1)

    up_first(up_chunks - 1)

    total = lg_acc[...]
    for s in range(1, n_tp):
        lg_copy(s).wait_recv()
        total = total + lg_recv[s - 1].astype(F32)
    total = jnp.where(live(total.shape), total, 0.0)
    lg_t[...] = total.T.astype(BF16)

    @pl.loop(0, down_chunks)
    def _(c):
        hidden_copy(c).wait()
        block = lax.dot_general(
            lg_t[...], hidden_v[c % 2].reshape(rows, down_width),
            (((1,), (0,)), ((), ())), preferred_element_type=F32)
        dn[c] = block.astype(BF16).reshape(dn.shape[1:])
        dn_copy(0, c).start()

        @pl.when(c + 2 < down_chunks)
        def _():
            hidden_copy(c + 2).start()

        @pl.when(c > 0)
        def _():
            dn_pass(0, c - 1)

    dn_pass(0, down_chunks - 1)

    last = len(steps) - 1

    @pl.loop(0, up_chunks + last - 1)
    def _(t):
        for k in range(1, last + 1):
            c = t - (k - 1)

            @pl.when((c >= 0) & (c < up_chunks))
            def _():
                if k < last:
                    up_pass(k, c)
                else:
                    at = pl.ds(pl.multiple_of(c * width, width), width)
                    up_out[:, at] = up_add(k, c)

    for k in range(1, n_dp_steps - 1):
        @pl.loop(0, down_chunks)
        def _(c):
            dn_pass(k, c)

    @pl.loop(0, down_chunks)
    def _(c):
        share = dn_add(n_dp_steps - 1, c)
        at = pl.ds(pl.multiple_of(c * down_width, down_width), down_width)

        @pl.when(mb == 0)
        def _():
            pre_s[c] = share.astype(BF16)
            pre_copy(c).start()
            run_out[0, at, :] = share.T

        @pl.when(mb > 0)
        def _():
            pre_copy(c).wait_recv()
            running = share + pre_r[c].astype(F32)

            @pl.when(mb < n_mb - 1)
            def _():
                pre_s[c] = running.astype(BF16)
                pre_copy(c).start()

            run_out[0, at, :] = running.T

    for s in range(1, n_tp):
        lat_copy(s).wait_send()
        lg_copy(s).wait_send()

    @pl.loop(0, up_chunks)
    def _(c):
        for k in range(len(steps)):
            up_copy(k, c).wait_send()

    @pl.loop(0, down_chunks)
    def _(c):
        for k in range(n_dp_steps):
            dn_copy(k, c).wait_send()

        @pl.when(mb < n_mb - 1)
        def _():
            pre_copy(c).wait_send()


def local(sizes, hidden, latent, out_grad, up_weight, mb_tokens, slot_mb):
    n_mb, n_tp, n_dp = sizes
    _, slot_count, cap, feature_part = hidden.shape
    rank_part = latent.shape[3]
    rank, column_part = up_weight.shape
    rows = slot_count * cap
    width = column_part // UP_CHUNKS
    down_width = feature_part // DOWN_CHUNKS
    dp_bits, mb_bits = bits_of(n_dp), bits_of(n_mb)
    bits = dp_bits + mb_bits
    up_rows = rank >> bits
    share = rank >> dp_bits
    dma = pltpu.SemaphoreType.DMA
    scratch = [
        pltpu.VMEM((UP_CHUNKS, slot_count, cap, width), BF16),
        pltpu.VMEM((2, rank, width), BF16),
        pltpu.VMEM((2, slot_count, cap, down_width), BF16),
        pltpu.VMEM((n_tp, slot_count, cap, rank_part), BF16),
        pltpu.VMEM((n_tp, rank_part, rows), BF16),
        pltpu.VMEM((rows, rank), F32),
        pltpu.VMEM((rows, rank), BF16),
        pltpu.VMEM((n_tp - 1, rows, rank), BF16),
        pltpu.VMEM((rank, rows), BF16),
        pltpu.VMEM((UP_CHUNKS,) + (2,) * bits + (up_rows, width), BF16),
        [pltpu.VMEM((UP_CHUNKS,) + (2,) * (bits - 1 - k) + (up_rows, width), BF16) for k in range(bits)],
        pltpu.VMEM((DOWN_CHUNKS,) + (2,) * dp_bits + (share, down_width), BF16),
        [pltpu.VMEM((DOWN_CHUNKS,) + (2,) * (dp_bits - 1 - k) + (share, down_width), BF16) for k in range(dp_bits)],
        pltpu.VMEM((DOWN_CHUNKS, share, down_width), BF16),
        pltpu.VMEM((DOWN_CHUNKS, share, down_width), BF16),
        dma((UP_CHUNKS,)), dma((2,)), dma((2,)), dma,
        dma((n_tp - 1,)), dma((n_tp - 1,)), dma((n_tp - 1,)), dma((n_tp - 1,)),
        dma((bits, UP_CHUNKS)), dma((bits, UP_CHUNKS)),
        dma((dp_bits, DOWN_CHUNKS)), dma((dp_bits, DOWN_CHUNKS)),
        dma((DOWN_CHUNKS,)), dma((DOWN_CHUNKS,)),
    ]
    hbm = pl.BlockSpec(memory_space=pl.ANY)
    smem = pl.BlockSpec(memory_space=pltpu.SMEM)
    vmem = pl.BlockSpec(memory_space=pltpu.VMEM)
    return pl.pallas_call(
        functools.partial(kernel, sizes),
        out_shape=(
            jax.ShapeDtypeStruct((up_rows, column_part), F32),
            jax.ShapeDtypeStruct((1, feature_part, share), F32),
        ),
        in_specs=[hbm] * 4 + [smem] * 2,
        out_specs=(vmem, vmem),
        scratch_shapes=scratch,
        compiler_params=pltpu.CompilerParams(
            collective_id=0, has_side_effects=True, vmem_limit_bytes=67043328),
    )(hidden, latent, out_grad, up_weight, mb_tokens, slot_mb)


def solution(mesh):
    sizes = tuple(mesh.shape[axis] for axis in ("mb", "tp", "dp"))
    return jax.shard_map(
        functools.partial(local, sizes),
        mesh=mesh,
        in_specs=(
            P("dp", "mb", None, "tp"),
            P("dp", "mb", None, "tp"),
            P("dp", "mb", None, "tp"),
            P(None, "tp"),
            P("dp", None),
            P("dp", "mb"),
        ),
        out_specs=(P(("mb", "dp"), "tp"), P("mb", "tp", "dp")),
        check_vma=False,
    )
```

```python
import functools

import jax
import jax.numpy as jnp
from jax import lax
from jax.experimental import pallas as pl
from jax.experimental.pallas import tpu as pltpu
from jax.sharding import PartitionSpec as P

F32 = jnp.float32
BF16 = jnp.bfloat16
UP_CHUNKS = 8
DOWN_CHUNKS = 7


def bits_of(size):
    count = size.bit_length() - 1
    assert size == 1 << count, "axis size"
    return count


def kernel(sizes, hidden, latent, grad, weight, tokens, slots, up_out, run_out,
           grad_v, weight_v, hidden_v, lat_v, lat_t, lg_acc, lg_send, lg_recv, lg_t,
           up, up_r, dn, dn_r, pre_r, pre_s,
           grad_sem, weight_sem, hidden_sem, lat_sem, lat_ss, lat_rs, lg_ss, lg_rs,
           up_ss, up_rs, dn_ss, dn_rs, pre_ss, pre_rs):
    n_mb, n_tp, n_dp = sizes
    mb, tp, dp = (lax.axis_index(a) for a in ("mb", "tp", "dp"))
    up_chunks, slot_count, cap, width = grad_v.shape
    rows = slot_count * cap
    rank_part = lat_v.shape[-1]
    down_chunks, down_width = dn.shape[0], dn.shape[-1]

    steps = []
    for axis, index, size in (("dp", dp, n_dp), ("mb", mb, n_mb)):
        for k in range(bits_of(size)):
            bit = (index // (1 << k)) % 2
            steps.append((bit, {axis: index + (1 - 2 * bit) * (1 << k)}))
    n_dp_steps = bits_of(n_dp)
    tp_peers = [{"tp": (tp + s) % n_tp} for s in range(1, n_tp)]
    following, preceding = {"mb": (mb + 1) % n_mb}, {"mb": (mb + n_mb - 1) % n_mb}

    def grad_copy(c):
        return pltpu.make_async_copy(
            grad.at[0, :, :, pl.ds(pl.multiple_of(c * width, width), width)], grad_v.at[c], grad_sem.at[c])

    def weight_copy(c):
        return pltpu.make_async_copy(
            weight.at[:, pl.ds(pl.multiple_of(c * width, width), width)], weight_v.at[c % 2], weight_sem.at[c % 2])

    def hidden_copy(c):
        return pltpu.make_async_copy(
            hidden.at[0, :, :, pl.ds(pl.multiple_of(c * down_width, down_width), down_width)],
            hidden_v.at[c % 2], hidden_sem.at[c % 2])

    def remote(src, dst, ss, rs, to):
        return pltpu.make_async_remote_copy(
            src_ref=src, dst_ref=dst, send_sem=ss, recv_sem=rs,
            device_id=to, device_id_type=pl.DeviceIdType.MESH)

    own_latent = pltpu.make_async_copy(latent.at[0], lat_v.at[0], lat_sem)
    own_latent.start()
    for c in range(2):
        weight_copy(c).start()
        hidden_copy(c).start()

    @pl.loop(0, up_chunks)
    def _(c):
        grad_copy(c).start()

    barrier = pltpu.get_barrier_semaphore()
    greeted = [to for _, to in steps] + tp_peers + [following, preceding]
    for to in greeted:
        pl.semaphore_signal(barrier, inc=1, device_id=to, device_id_type=pl.DeviceIdType.MESH)
    pl.semaphore_wait(barrier, len(greeted))

    def lat_copy(s):
        return remote(latent.at[0], lat_v.at[s], lat_ss.at[s - 1], lat_rs.at[s - 1], tp_peers[s - 1])

    def lg_copy(s):
        return remote(lg_send, lg_recv.at[s - 1], lg_ss.at[s - 1], lg_rs.at[s - 1], tp_peers[s - 1])

    for s in range(1, n_tp):
        lat_copy(s).start()

    tp_bits = bits_of(n_tp)
    last = len(steps) - 1
    part_steps = len(steps) - tp_bits

    def part_at(s):
        part = (tp + n_tp - s) % n_tp
        return tuple((part // (1 << k)) % 2 for k in reversed(range(tp_bits)))

    def up_copy(k, s, c):
        bit, to = steps[k]
        head = (c,) + (part_at(s) if k < part_steps else ())
        free = len(steps) - 1 - k - (len(head) - 1)
        src = (up if k == 0 else up_r[k - 1]).at[head + (slice(None),) * free + (1 - bit,)]
        return remote(src, up_r[k].at[head], up_ss.at[k, s, c], up_rs.at[k, s, c], to)

    def up_add(k, s, c):
        bit, _ = steps[k]
        head = (c,) + (part_at(s) if k < part_steps else ())
        free = len(steps) - 1 - k - (len(head) - 1)
        up_copy(k, s, c).wait_recv()
        kept = (up if k == 0 else up_r[k - 1])[head + (slice(None),) * free + (bit,)]
        return kept.astype(F32) + up_r[k][head].astype(F32)

    def up_pass(k, s, c):
        head = (c,) + (part_at(s) if k < part_steps else ())
        up_r[k][head] = up_add(k, s, c).astype(BF16)
        if k + 1 != part_steps:
            up_copy(k + 1, s, c).start()

    def up_make(s, c):
        block = lax.dot_general(
            lat_t[s], grad_v[c].reshape(rows, width),
            (((1,), (0,)), ((), ())), preferred_element_type=F32).astype(BF16)
        head = (c,) + part_at(s)
        up[head] = block.reshape(up.shape[1 + tp_bits:])
        up_copy(0, s, c).start()

    def up_tick(t):
        for k in range(1, last + 1):
            c = t - (k - 1)

            @pl.when((c >= 0) & (c < up_chunks))
            def _():
                if k < part_steps:
                    for s in range(1 if k == 1 else 0, n_tp):
                        up_pass(k, s, c)
                    if k + 1 == part_steps:
                        up_copy(part_steps, 0, c).start()
                elif k < last:
                    up_pass(k, 0, c)
                else:
                    at = pl.ds(pl.multiple_of(c * width, width), width)
                    up_out[:, at] = up_add(k, 0, c)

    def latent_part(s):
        part = lat_v[s].reshape(rows, rank_part).astype(F32)
        part = jnp.where(live(part.shape), part, 0.0)
        lat_t[s] = part.T.astype(BF16)

    def dn_copy(k, c):
        bit, to = steps[k]
        src = (dn if k == 0 else dn_r[k - 1]).at[c]
        index = (slice(None),) * (n_dp_steps - 1 - k) + (1 - bit,)
        return remote(src.at[index], dn_r[k].at[c], dn_ss.at[k, c], dn_rs.at[k, c], to)

    def dn_add(k, c):
        bit, _ = steps[k]
        dn_copy(k, c).wait_recv()
        src = dn if k == 0 else dn_r[k - 1]
        kept = src[(c,) + (slice(None),) * (n_dp_steps - 1 - k) + (bit,)]
        return kept.astype(F32) + dn_r[k][c].astype(F32)

    def dn_pass(k, c):
        dn_r[k][c] = dn_add(k, c).astype(BF16)
        dn_copy(k + 1, c).start()

    def pre_copy(c):
        return remote(pre_s.at[c], pre_r.at[c], pre_ss.at[c], pre_rs.at[c], following)

    counts = [tokens[0, slots[0, s]] for s in range(slot_count)]

    def live(shape):
        row = lax.broadcasted_iota(jnp.int32, shape, 0)
        valid = row < counts[0]
        for s in range(1, slot_count):
            valid = valid | ((row >= s * cap) & (row < s * cap + counts[s]))
        return valid

    own_latent.wait()
    latent_part(0)

    @pl.loop(0, up_chunks)
    def _(c):
        grad_copy(c).wait()
        up_make(0, c)

        @pl.when(c > 0)
        def _():
            up_pass(0, 0, c - 1)

    up_pass(0, 0, up_chunks - 1)

    lg_acc[...] = jnp.zeros_like(lg_acc)

    @pl.loop(0, up_chunks)
    def _(c):
        weight_copy(c).wait()
        lg_acc[...] += lax.dot_general(
            grad_v[c].reshape(rows, width), weight_v[c % 2], (((1,), (1,)), ((), ())),
            preferred_element_type=F32)

        @pl.when(c + 2 < up_chunks)
        def _():
            weight_copy(c + 2).start()

        @pl.when(c > 0)
        def _():
            up_pass(1, 0, c - 1)

    lg_send[...] = lg_acc[...].astype(BF16)
    for s in range(1, n_tp):
        lg_copy(s).start()

    for s in range(1, n_tp):
        lat_copy(s).wait_recv()
        latent_part(s)

        @pl.loop(0, up_chunks)
        def _(c):
            up_make(s, c)

            @pl.when(c > 0)
            def _():
                up_pass(0, s, c - 1)

        up_pass(0, s, up_chunks - 1)

    up_pass(1, 0, up_chunks - 1)
    early = up_chunks - 2

    @pl.loop(0, early)
    def _(t):
        up_tick(t)

    total = lg_acc[...]
    for s in range(1, n_tp):
        lg_copy(s).wait_recv()
        total = total + lg_recv[s - 1].astype(F32)
    total = jnp.where(live(total.shape), total, 0.0)
    lg_t[...] = total.T.astype(BF16)

    @pl.loop(0, down_chunks)
    def _(c):
        hidden_copy(c).wait()
        block = lax.dot_general(
            lg_t[...], hidden_v[c % 2].reshape(rows, down_width),
            (((1,), (0,)), ((), ())), preferred_element_type=F32)
        dn[c] = block.astype(BF16).reshape(dn.shape[1:])
        dn_copy(0, c).start()

        @pl.when(c + 2 < down_chunks)
        def _():
            hidden_copy(c + 2).start()

        @pl.when(c > 0)
        def _():
            dn_pass(0, c - 1)

    dn_pass(0, down_chunks - 1)

    @pl.loop(early, up_chunks + last - 1)
    def _(t):
        up_tick(t)

    for k in range(1, n_dp_steps - 1):
        @pl.loop(0, down_chunks)
        def _(c):
            dn_pass(k, c)

    @pl.loop(0, down_chunks)
    def _(c):
        share = dn_add(n_dp_steps - 1, c)
        at = pl.ds(pl.multiple_of(c * down_width, down_width), down_width)

        @pl.when(mb == 0)
        def _():
            pre_s[c] = share.astype(BF16)
            pre_copy(c).start()
            run_out[0, at, :] = share.T

        @pl.when(mb > 0)
        def _():
            pre_copy(c).wait_recv()
            running = share + pre_r[c].astype(F32)

            @pl.when(mb < n_mb - 1)
            def _():
                pre_s[c] = running.astype(BF16)
                pre_copy(c).start()

            run_out[0, at, :] = running.T

    for s in range(1, n_tp):
        lat_copy(s).wait_send()
        lg_copy(s).wait_send()

    @pl.loop(0, up_chunks)
    def _(c):
        for k in range(len(steps)):
            for s in range(n_tp if k < part_steps else 1):
                up_copy(k, s, c).wait_send()

    @pl.loop(0, down_chunks)
    def _(c):
        for k in range(n_dp_steps):
            dn_copy(k, c).wait_send()

        @pl.when(mb < n_mb - 1)
        def _():
            pre_copy(c).wait_send()


def local(sizes, hidden, latent, out_grad, up_weight, mb_tokens, slot_mb):
    n_mb, n_tp, n_dp = sizes
    _, slot_count, cap, feature_part = hidden.shape
    rank_part = latent.shape[3]
    rank, column_part = up_weight.shape
    rows = slot_count * cap
    width = column_part // UP_CHUNKS
    down_width = feature_part // DOWN_CHUNKS
    dp_bits, mb_bits = bits_of(n_dp), bits_of(n_mb)
    bits = dp_bits + mb_bits
    up_rows = rank >> bits
    share = rank >> dp_bits
    dma = pltpu.SemaphoreType.DMA
    scratch = [
        pltpu.VMEM((UP_CHUNKS, slot_count, cap, width), BF16),
        pltpu.VMEM((2, rank, width), BF16),
        pltpu.VMEM((2, slot_count, cap, down_width), BF16),
        pltpu.VMEM((n_tp, slot_count, cap, rank_part), BF16),
        pltpu.VMEM((n_tp, rank_part, rows), BF16),
        pltpu.VMEM((rows, rank), F32),
        pltpu.VMEM((rows, rank), BF16),
        pltpu.VMEM((n_tp - 1, rows, rank), BF16),
        pltpu.VMEM((rank, rows), BF16),
        pltpu.VMEM((UP_CHUNKS,) + (2,) * bits + (up_rows, width), BF16),
        [pltpu.VMEM((UP_CHUNKS,) + (2,) * (bits - 1 - k) + (up_rows, width), BF16) for k in range(bits)],
        pltpu.VMEM((DOWN_CHUNKS,) + (2,) * dp_bits + (share, down_width), BF16),
        [pltpu.VMEM((DOWN_CHUNKS,) + (2,) * (dp_bits - 1 - k) + (share, down_width), BF16) for k in range(dp_bits)],
        pltpu.VMEM((DOWN_CHUNKS, share, down_width), BF16),
        pltpu.VMEM((DOWN_CHUNKS, share, down_width), BF16),
        dma((UP_CHUNKS,)), dma((2,)), dma((2,)), dma,
        dma((n_tp - 1,)), dma((n_tp - 1,)), dma((n_tp - 1,)), dma((n_tp - 1,)),
        dma((bits, n_tp, UP_CHUNKS)), dma((bits, n_tp, UP_CHUNKS)),
        dma((dp_bits, DOWN_CHUNKS)), dma((dp_bits, DOWN_CHUNKS)),
        dma((DOWN_CHUNKS,)), dma((DOWN_CHUNKS,)),
    ]
    hbm = pl.BlockSpec(memory_space=pl.ANY)
    smem = pl.BlockSpec(memory_space=pltpu.SMEM)
    vmem = pl.BlockSpec(memory_space=pltpu.VMEM)
    return pl.pallas_call(
        functools.partial(kernel, sizes),
        out_shape=(
            jax.ShapeDtypeStruct((up_rows, column_part), F32),
            jax.ShapeDtypeStruct((1, feature_part, share), F32),
        ),
        in_specs=[hbm] * 4 + [smem] * 2,
        out_specs=(vmem, vmem),
        scratch_shapes=scratch,
        compiler_params=pltpu.CompilerParams(
            collective_id=0, has_side_effects=True, vmem_limit_bytes=67043328),
    )(hidden, latent, out_grad, up_weight, mb_tokens, slot_mb)


def solution(mesh):
    sizes = tuple(mesh.shape[axis] for axis in ("mb", "tp", "dp"))
    return jax.shard_map(
        functools.partial(local, sizes),
        mesh=mesh,
        in_specs=(
            P("dp", "mb", None, "tp"),
            P("dp", "mb", None, "tp"),
            P("dp", "mb", None, "tp"),
            P(None, "tp"),
            P("dp", None),
            P("dp", "mb"),
        ),
        out_specs=(P(("mb", "dp"), "tp"), P("mb", "tp", "dp")),
        check_vma=False,
    )
```
